256 devices in a mesh: beam: 16 (over x_hi, y, core), tm: 16 (over z, x_lo).
Axes of the slice: x: 4 (x_hi: 2, x_lo: 2; x = x_hi * 2 + x_lo), y: 4, z: 8, core: 2. Of those that a mesh axis runs over, the one named last changes fastest.
Arguments:
- samples: float32 [2, 150994944], P(None, ('beam', 'tm')), parts along dimension 1, may hold values from -6 to 6
- prototype: float32 [16, 4096], replicated, may hold values from -1.5 to 1.5
Outputs:
- spectra: bfloat16 [2, 49152, 4096], P(None, 'beam', 'tm'), parts along dimension 1
The draws below stay inside these ranges and needn't reach their ends.
There are 16 independent parts, one for each index of `beam`. The reference program is written for one: setup_inputs(seed, part) draws one part's arguments, and reference() takes and returns one part's arrays. A program takes and returns all parts, laid end to end along the dimension named above; an argument that names none is the same for every part. Nothing has to cross between parts.
All inputs are finite; a program needn't handle non-finite values.
Results may differ from the reference program's by a relative error of at most 0.001.
Values may be sent and summed in bfloat16 or wider, within the bound.
A program may use at most 128 MiB of HBM per device.

```python
import math
import jax
import jax.numpy as jnp

CHANNELS = 4096
TAPS = 16
HOP = 3072
FRAMES = 3072
SAMPLES = 9437184


def steps_of(rng, extent, shards, low, top_value):
    factor_of = 1.0
    for axis_at, blocks in shards:
        draws = jax.random.uniform(jax.random.fold_in(jax.random.fold_in(rng, 6), axis_at), (blocks,), jnp.float32, low / len(shards), top_value / len(shards))
        factor_of = factor_of * jnp.repeat(jnp.exp(draws), extent[axis_at] // blocks).reshape((-1,) + (1,) * (len(extent) - 1 - axis_at))
    return factor_of


def noise(own_key, dims, scale, limit, shards=(), held_as=jnp.bfloat16):
    result = jax.random.normal(own_key, dims, jnp.float32) * scale
    if len(shards) > 0:
        result = steps_of(own_key, dims, shards, -0.22, 0.18) * result
    return jnp.clip(result, min=-limit, max=limit).astype(held_as)


def setup_inputs(seed: int = 0, part: int = 0) -> dict:
    key_list = jax.random.split(jax.random.key(seed), 3)
    part_keys = jax.random.split(jax.random.fold_in(key_list[2], part), 3)
    return {
        "samples": noise(part_keys[0], (2, SAMPLES), 1.0, 6.0, ((1, 16),), jnp.float32),
        "prototype": noise(key_list[1], (TAPS, CHANNELS), TAPS ** -0.5, 1.5, (), jnp.float32),
    }


def reference(samples, prototype):
    window = TAPS * CHANNELS
    zeros_front = jnp.zeros((2, window - HOP), samples.dtype)
    extended = jnp.concatenate([zeros_front, samples], axis=1)
    signal = extended[0] + 1j * extended[1]
    frame_ids = jnp.arange(FRAMES).astype(jnp.int32)
    phase_ids = jnp.arange(CHANNELS).astype(jnp.int32)
    folded = jnp.zeros((FRAMES, CHANNELS), signal.dtype)
    for tap_index in range(TAPS):
        starts = frame_ids * HOP + tap_index * CHANNELS
        index_grid = (starts[:, None] + phase_ids[None, :]).astype(jnp.int32)
        folded = folded + prototype[tap_index][None, :] * signal[index_grid]
    transformed = jnp.fft.fft(folded, axis=1)
    rotation = (frame_ids + 1) * HOP % CHANNELS
    turns = phase_ids[None, :] * rotation[:, None] % CHANNELS
    angle = 2.0 * math.pi * turns.astype(samples.dtype) / CHANNELS
    factor = (jnp.cos(angle) - 1j * jnp.sin(angle)) / math.sqrt(CHANNELS)
    spectrum = transformed * factor
    return jnp.stack([jnp.real(spectrum), jnp.imag(spectrum)]).astype(jnp.bfloat16)
```

```python
import math

import jax
import jax.numpy as jnp
import numpy as np
from jax import lax
from jax.experimental import pallas as pl
from jax.experimental.pallas import tpu as pltpu
from jax.sharding import PartitionSpec as P

CHANNELS = 4096
TAPS = 16
HOP = 3072
LANES = 128
ROWS = 32
PEERS = 16
FRAME_ROWS = 2 * ROWS
HOP_ROWS = 2 * HOP // LANES
RIM_ROWS = 2 * (TAPS * CHANNELS - HOP) // LANES
STEP = 16
MESH = pl.DeviceIdType.MESH
OFFSETS = [(dz, dx) for dz in (1, -1, 2, -2, 3, -3, 4) for dx in (0, 1)] + [(0, 1)]


def split_bf16(table):
    high = table.astype(np.float32).astype(jnp.bfloat16)
    low = (table - high.astype(np.float64)).astype(np.float32).astype(jnp.bfloat16)
    return high, low


def first_matrix():
    a = np.arange(ROWS)
    table = np.zeros((2, 4, ROWS, 4, ROWS, 2))
    for frame in range(4):
        turns = (-np.outer(a, a) + 8 * a[:, None] * (frame + 1)) % 32
        unit = np.exp(2j * np.pi * turns / 32) / 64
        table[0, frame, :, frame, :, 0] = unit.real
        table[0, frame, :, frame, :, 1] = -unit.imag
        table[1, frame, :, frame, :, 0] = unit.imag
        table[1, frame, :, frame, :, 1] = unit.real
    return split_bf16(table.reshape(256, 256))


def middle_tables():
    turns = np.outer(np.arange(ROWS), np.arange(LANES))
    angle = 2 * np.pi * turns / CHANNELS
    tables = np.stack([np.cos(angle), np.sin(angle)])
    return np.tile(tables, (1, 4, 1)).reshape(256, LANES).astype(np.float32)


def second_matrix():
    k_l = (8 * np.arange(16)[None, :] + np.arange(8)[:, None]).reshape(-1)
    angle = 2 * np.pi * (np.outer(k_l, np.arange(LANES)) % LANES) / LANES
    c, s = np.cos(angle), np.sin(angle)
    return split_bf16(np.block([[c, s], [-s, c]]))


def peer(me, dz, dx):
    return (me // 2 + dz + 8) % 8 * 2 + (me % 2 + dx) % 2


def dot3(left_high, left_low, right_high, right_low, dims):
    def one(a, b):
        return lax.dot_general(a, b, (dims, ((), ())), preferred_element_type=jnp.float32)

    return one(left_high, right_high) + one(left_high, right_low) + one(left_low, right_high)


def halves(value):
    high = value.astype(jnp.bfloat16)
    return high, (value - high.astype(jnp.float32)).astype(jnp.bfloat16)


def kernel(
    frames, x_hbm, h_hbm, one_hbm, mid_hbm, two_hbm, o_ref,
    x, h, one, mid, two, fold_high, fold_low, turn_high, turn_low, staged, ready,
    load_sem, rim_sem, send_sem, recv_sem,
):
    me = lax.axis_index("tm")
    local_rows = frames * HOP_ROWS
    steps = frames // STEP
    first_step = 2
    low_row = first_step * STEP * HOP_ROWS - RIM_ROWS
    high_row = ((first_step + 1) * STEP - 1) * HOP_ROWS + TAPS * FRAME_ROWS - RIM_ROWS

    barrier = pltpu.get_barrier_semaphore()
    for dz, dx in OFFSETS:
        pl.semaphore_signal(barrier, inc=1, device_id={"tm": peer(me, dz, dx)}, device_id_type=MESH)

    def load(index, start, stop):
        return pltpu.make_async_copy(
            x_hbm.at[pl.ds(start, stop - start)], x.at[pl.ds(RIM_ROWS + start, stop - start)], load_sem.at[index]
        )

    early = [
        load(0, low_row, high_row),
        pltpu.make_async_copy(h_hbm, h, load_sem.at[3]),
        pltpu.make_async_copy(one_hbm, one, load_sem.at[4]),
        pltpu.make_async_copy(mid_hbm, mid, load_sem.at[5]),
        pltpu.make_async_copy(two_hbm, two, load_sem.at[6]),
    ]
    late = [load(1, high_row, local_rows), load(2, 0, low_row)]
    for copy in early + late:
        copy.start()

    pl.semaphore_wait(barrier, len(OFFSETS))

    def rim_copy():
        return pltpu.make_async_remote_copy(
            x_hbm.at[pl.ds(local_rows - RIM_ROWS, RIM_ROWS)],
            x.at[pl.ds(0, RIM_ROWS)],
            rim_sem.at[0],
            rim_sem.at[1],
            device_id={"tm": lax.rem(me + 1, PEERS)},
            device_id_type=MESH,
        )

    @pl.when(me < PEERS - 1)
    def _():
        rim_copy().start()

    @pl.when(me == 0)
    def _():
        x[pl.ds(0, RIM_ROWS), :] = jnp.zeros((RIM_ROWS, LANES), jnp.float32)

    for copy in early:
        copy.wait()

    lane = lax.broadcasted_iota(jnp.int32, (16, LANES), 1)
    low_64 = lane < 64
    even_32 = lane // 32 % 2 == 0

    def exchange(tiles):
        a, b, c, d = tiles
        ac = jnp.where(low_64, a, pltpu.roll(c, 64, 1)), jnp.where(low_64, pltpu.roll(a, 64, 1), c)
        bd = jnp.where(low_64, b, pltpu.roll(d, 64, 1)), jnp.where(low_64, pltpu.roll(b, 64, 1), d)
        done = []
        for p, q in zip(ac, bd):
            done.append(jnp.where(even_32, p, pltpu.roll(q, 32, 1)))
            done.append(jnp.where(even_32, pltpu.roll(p, 96, 1), q))
        return done

    def eight_frames(first_frame, sub):
        base = first_frame * HOP_ROWS

        def fold(block, carry):
            at = pl.multiple_of(block * 16, 16)
            taps = [h[pl.ds(at + p * FRAME_ROWS, 16), :] for p in range(TAPS)]
            for f in range(8):
                total = None
                for p in range(TAPS):
                    rows = pl.ds(pl.multiple_of(base + f * HOP_ROWS + p * FRAME_ROWS + at, 16), 16)
                    term = taps[p] * x[rows, :]
                    total = term if total is None else total + term
                high, low = halves(total)
                place = pl.ds(pl.multiple_of(f % 4 * FRAME_ROWS + at, 16), 16)
                fold_high[place, f // 4 * LANES : (f // 4 + 1) * LANES] = high
                fold_low[place, f // 4 * LANES : (f // 4 + 1) * LANES] = low
            return carry

        lax.fori_loop(0, FRAME_ROWS // 16, fold, 0)

        section = dot3(one[0:256, :], one[256:512, :], fold_high[...], fold_low[...], ((1,), (0,)))
        cos_mid, sin_mid = mid[0:128, :], mid[128:256, :]
        for g in range(2):
            re = section[0:128, g * LANES : (g + 1) * LANES]
            im = section[128:256, g * LANES : (g + 1) * LANES]
            for part, value in enumerate((re * cos_mid + im * sin_mid, im * cos_mid - re * sin_mid)):
                high, low = halves(value)
                turn_high[g * 128 : (g + 1) * 128, part * LANES : (part + 1) * LANES] = high
                turn_low[g * 128 : (g + 1) * 128, part * LANES : (part + 1) * LANES] = low

        out = dot3(two[0:256, :], two[256:512, :], turn_high[...], turn_low[...], ((1,), (1,)))
        for part in range(2):
            for half in range(2):
                for side in range(2):
                    tiles = [
                        out[part * 128 + (half * 4 + q) * 16 : part * 128 + (half * 4 + q + 1) * 16,
                            side * LANES : (side + 1) * LANES]
                        for q in range(4)
                    ]
                    for r, tile in enumerate(exchange(tiles)):
                        staged[sub, part, half, pl.ds(side * 4 + r, 16, stride=8), :] = tile

    def step_body(i, carry):
        step = lax.rem(i + first_step, steps)

        @pl.when(i == 1)
        def _():
            for copy in late:
                copy.wait()

        @pl.when(jnp.logical_and(i == steps - first_step, me > 0))
        def _():
            rim_copy().wait_recv()

        for sub in range(2):
            eight_frames(step * STEP + sub * 8, sub)

        rows = pl.ds(pl.multiple_of(step * STEP, STEP), STEP)
        for c in range(PEERS):
            for part in range(2):
                for half in range(2):
                    pair = [staged[sub, part, half, c * 8 : (c + 1) * 8, :] for sub in range(2)]
                    ready[c, part, rows, half * LANES : (half + 1) * LANES] = jnp.concatenate(pair, axis=0).astype(
                        jnp.bfloat16
                    )

        there = pl.ds(pl.multiple_of(me * frames + step * STEP, STEP), STEP)
        for index, (dz, dx) in enumerate(OFFSETS):
            target = peer(me, dz, dx)
            pltpu.make_async_remote_copy(
                ready.at[target, :, rows],
                o_ref.at[:, there],
                send_sem.at[index],
                recv_sem.at[index],
                device_id={"tm": target},
                device_id_type=MESH,
            ).start()
        pltpu.make_async_copy(ready.at[me, :, rows], o_ref.at[:, there], send_sem.at[len(OFFSETS)]).start()
        return carry

    lax.fori_loop(0, steps, step_body, 0)

    @pl.when(me < PEERS - 1)
    def _():
        rim_copy().wait_send()

    mine = pl.ds(pl.multiple_of(me * frames, STEP), frames)
    pltpu.make_async_copy(ready.at[me], o_ref.at[:, mine], send_sem.at[len(OFFSETS)]).wait()
    for index, (dz, dx) in enumerate(OFFSETS):
        target = peer(me, dz, dx)
        source = peer(me, -dz, dx)
        here = pl.ds(pl.multiple_of(source * frames, STEP), frames)
        whole = pltpu.make_async_remote_copy(
            ready.at[target],
            o_ref.at[:, here],
            send_sem.at[index],
            recv_sem.at[index],
            device_id={"tm": target},
            device_id_type=MESH,
        )
        whole.wait_send()
        whole.wait_recv()


def local(samples, prototype):
    block_len = samples.shape[1]
    frames = block_len // HOP
    rows = 2 * block_len // LANES
    x = samples.reshape(2, block_len // LANES, LANES).transpose(1, 0, 2).reshape(rows, LANES)
    h = jnp.repeat(prototype.reshape(TAPS * ROWS, LANES), 2, axis=0)
    one = jnp.concatenate([jnp.asarray(part) for part in first_matrix()], axis=0)
    two = jnp.concatenate([jnp.asarray(part) for part in second_matrix()], axis=0)
    mid = jnp.asarray(middle_tables())
    width = CHANNELS // PEERS

    def body(*refs):
        kernel(frames, *refs)

    return pl.pallas_call(
        body,
        out_shape=jax.ShapeDtypeStruct((2, PEERS * frames, width), jnp.bfloat16),
        in_specs=[pl.BlockSpec(memory_space=pltpu.HBM)] * 5,
        out_specs=pl.BlockSpec(memory_space=pltpu.HBM),
        scratch_shapes=[
            pltpu.VMEM((RIM_ROWS + rows, LANES), jnp.float32),
            pltpu.VMEM((TAPS * FRAME_ROWS, LANES), jnp.float32),
            pltpu.VMEM((512, 256), jnp.bfloat16),
            pltpu.VMEM((256, LANES), jnp.float32),
            pltpu.VMEM((512, 256), jnp.bfloat16),
            pltpu.VMEM((256, 256), jnp.bfloat16),
            pltpu.VMEM((256, 256), jnp.bfloat16),
            pltpu.VMEM((256, 256), jnp.bfloat16),
            pltpu.VMEM((256, 256), jnp.bfloat16),
            pltpu.VMEM((2, 2, 2, 128, LANES), jnp.float32),
            pltpu.VMEM((PEERS, 2, frames, width), jnp.bfloat16),
            pltpu.SemaphoreType.DMA((7,)),
            pltpu.SemaphoreType.DMA((2,)),
            pltpu.SemaphoreType.DMA((len(OFFSETS) + 1,)),
            pltpu.SemaphoreType.DMA((len(OFFSETS),)),
        ],
        compiler_params=pltpu.CompilerParams(
            collective_id=0, has_side_effects=True, vmem_limit_bytes=60 * 1024 * 1024
        ),
    )(x, h, one, mid, two)


def solution(mesh):
    placed = (P(None, ("beam", "tm")), P())
    return jax.shard_map(
        local, mesh=mesh, in_specs=placed, out_specs=P(None, "beam", "tm"), check_vma=False
    )
```

```python
import math

import jax
import jax.numpy as jnp
import numpy as np
from jax import lax
from jax.experimental import pallas as pl
from jax.experimental.pallas import tpu as pltpu
from jax.sharding import PartitionSpec as P

CHANNELS = 4096
TAPS = 16
HOP = 3072
LANES = 128
ROWS = 32
PEERS = 16
FRAME_ROWS = 2 * ROWS
HOP_ROWS = 2 * HOP // LANES
RIM_ROWS = 2 * (TAPS * CHANNELS - HOP) // LANES
STEP = 16
MESH = pl.DeviceIdType.MESH
OFFSETS = [(dz, dx) for dz in (4, 3, -3, 2, -2, 1, -1) for dx in (1, 0)] + [(0, 1)]


def split_bf16(table):
    high = table.astype(np.float32).astype(jnp.bfloat16)
    low = (table - high.astype(np.float64)).astype(np.float32).astype(jnp.bfloat16)
    return high, low


def first_matrix():
    a = np.arange(ROWS)
    table = np.zeros((2, 4, ROWS, 4, ROWS, 2))
    for frame in range(4):
        turns = (-np.outer(a, a) + 8 * a[:, None] * (frame + 1)) % 32
        unit = np.exp(2j * np.pi * turns / 32) / 64
        table[0, frame, :, frame, :, 0] = unit.real
        table[0, frame, :, frame, :, 1] = -unit.imag
        table[1, frame, :, frame, :, 0] = unit.imag
        table[1, frame, :, frame, :, 1] = unit.real
    return split_bf16(table.reshape(256, 256))


def middle_tables():
    turns = np.outer(np.arange(ROWS), np.arange(LANES))
    angle = 2 * np.pi * turns / CHANNELS
    tables = np.stack([np.cos(angle), np.sin(angle)])
    return np.tile(tables, (1, 4, 1)).reshape(256, LANES).astype(np.float32)


def second_matrix():
    k_l = (8 * np.arange(16)[None, :] + np.arange(8)[:, None]).reshape(-1)
    angle = 2 * np.pi * (np.outer(k_l, np.arange(LANES)) % LANES) / LANES
    c, s = np.cos(angle), np.sin(angle)
    return split_bf16(np.block([[c, s], [-s, c]]))


def peer(me, dz, dx):
    return (me // 2 + dz + 8) % 8 * 2 + (me % 2 + dx) % 2


def dot3(left_high, left_low, right_high, right_low, dims):
    def one(a, b):
        return lax.dot_general(a, b, (dims, ((), ())), preferred_element_type=jnp.float32)

    return one(left_high, right_high) + one(left_high, right_low) + one(left_low, right_high)


def halves(value):
    high = value.astype(jnp.bfloat16)
    return high, (value - high.astype(jnp.float32)).astype(jnp.bfloat16)


def kernel(
    frames, x_hbm, h_hbm, one_hbm, mid_hbm, two_hbm, o_ref,
    x, rim_relay, taps_in, h, one, mid, two, fold_high, fold_low, turn_high, turn_low, staged, ready,
    load_sem, rim_sem, send_sem, recv_sem,
):
    me = lax.axis_index("tm")
    local_rows = frames * HOP_ROWS
    steps = frames // STEP
    first_step = 2
    low_row = first_step * STEP * HOP_ROWS - RIM_ROWS
    high_row = ((first_step + 1) * STEP - 1) * HOP_ROWS + TAPS * FRAME_ROWS - RIM_ROWS

    barrier = pltpu.get_barrier_semaphore()
    for dz, dx in OFFSETS:
        pl.semaphore_signal(barrier, inc=1, device_id={"tm": peer(me, dz, dx)}, device_id_type=MESH)

    def load(index, start, stop):
        return pltpu.make_async_copy(
            x_hbm.at[pl.ds(start, stop - start)], x.at[pl.ds(RIM_ROWS + start, stop - start)], load_sem.at[index]
        )

    early = [
        load(0, low_row, high_row),
        pltpu.make_async_copy(h_hbm, taps_in, load_sem.at[3]),
        pltpu.make_async_copy(one_hbm, one, load_sem.at[4]),
        pltpu.make_async_copy(mid_hbm, mid, load_sem.at[5]),
        pltpu.make_async_copy(two_hbm, two, load_sem.at[6]),
    ]
    late = [load(1, high_row, local_rows), load(2, 0, low_row)]
    for copy in early + late:
        copy.start()

    half_rim = RIM_ROWS // 2
    rim_start = local_rows - RIM_ROWS

    def rim(index, source, place, steps_on):
        return pltpu.make_async_remote_copy(
            source,
            place,
            rim_sem.at[0, index],
            rim_sem.at[1, index],
            device_id={"tm": lax.rem(me + steps_on + PEERS, PEERS)},
            device_id_type=MESH,
        )

    rim_whole = rim(0, x_hbm.at[pl.ds(rim_start, RIM_ROWS)], x.at[pl.ds(0, RIM_ROWS)], 1)
    rim_direct = rim(1, x_hbm.at[pl.ds(rim_start, half_rim)], x.at[pl.ds(0, half_rim)], 1)
    rim_aside = rim(2, x_hbm.at[pl.ds(rim_start + half_rim, half_rim)], rim_relay, -1)
    rim_onward = rim(3, rim_relay, x.at[pl.ds(half_rim, half_rim)], 2)
    odd = lax.rem(me, 2) == 1
    even = lax.rem(me, 2) == 0
    odd_sends = jnp.logical_and(odd, me < PEERS - 1)
    even_relays = jnp.logical_and(even, me < PEERS - 2)
    even_gets = jnp.logical_and(even, me > 0)

    pl.semaphore_wait(barrier, len(OFFSETS))

    @pl.when(even)
    def _():
        rim_whole.start()

    @pl.when(odd_sends)
    def _():
        rim_direct.start()
        rim_aside.start()

    for copy in early:
        copy.wait()

    for a in range(ROWS):
        for part in range(2):
            h[pl.ds(2 * a + part, TAPS, stride=FRAME_ROWS), :] = taps_in[:, a * LANES : (a + 1) * LANES]

    lane = lax.broadcasted_iota(jnp.int32, (16, LANES), 1)
    low_64 = lane < 64
    even_32 = lane // 32 % 2 == 0

    def exchange(tiles):
        a, b, c, d = tiles
        ac = jnp.where(low_64, a, pltpu.roll(c, 64, 1)), jnp.where(low_64, pltpu.roll(a, 64, 1), c)
        bd = jnp.where(low_64, b, pltpu.roll(d, 64, 1)), jnp.where(low_64, pltpu.roll(b, 64, 1), d)
        done = []
        for p, q in zip(ac, bd):
            done.append(jnp.where(even_32, p, pltpu.roll(q, 32, 1)))
            done.append(jnp.where(even_32, pltpu.roll(p, 96, 1), q))
        return done

    def eight_frames(first_frame, sub):
        base = first_frame * HOP_ROWS

        def fold(block, carry):
            at = pl.multiple_of(block * 16, 16)
            taps = [h[pl.ds(at + p * FRAME_ROWS, 16), :] for p in range(TAPS)]
            for f in range(8):
                total = None
                for p in range(TAPS):
                    rows = pl.ds(pl.multiple_of(base + f * HOP_ROWS + p * FRAME_ROWS + at, 16), 16)
                    term = taps[p] * x[rows, :]
                    total = term if total is None else total + term
                high, low = halves(total)
                place = pl.ds(pl.multiple_of(f % 4 * FRAME_ROWS + at, 16), 16)
                fold_high[place, f // 4 * LANES : (f // 4 + 1) * LANES] = high
                fold_low[place, f // 4 * LANES : (f // 4 + 1) * LANES] = low
            return carry

        lax.fori_loop(0, FRAME_ROWS // 16, fold, 0)

        section = dot3(one[0:256, :], one[256:512, :], fold_high[...], fold_low[...], ((1,), (0,)))
        cos_mid, sin_mid = mid[0:128, :], mid[128:256, :]
        for g in range(2):
            re = section[0:128, g * LANES : (g + 1) * LANES]
            im = section[128:256, g * LANES : (g + 1) * LANES]
            for part, value in enumerate((re * cos_mid + im * sin_mid, im * cos_mid - re * sin_mid)):
                high, low = halves(value)
                turn_high[g * 128 : (g + 1) * 128, part * LANES : (part + 1) * LANES] = high
                turn_low[g * 128 : (g + 1) * 128, part * LANES : (part + 1) * LANES] = low

        out = dot3(two[0:256, :], two[256:512, :], turn_high[...], turn_low[...], ((1,), (1,)))
        for part in range(2):
            for half in range(2):
                for side in range(2):
                    tiles = [
                        out[part * 128 + (half * 4 + q) * 16 : part * 128 + (half * 4 + q + 1) * 16,
                            side * LANES : (side + 1) * LANES]
                        for q in range(4)
                    ]
                    for r, tile in enumerate(exchange(tiles)):
                        staged[sub, part, half, pl.ds(side * 4 + r, 16, stride=8), :] = tile

    def compute(step):
        for sub in range(2):
            eight_frames(step * STEP + sub * 8, sub)

        rows = pl.ds(pl.multiple_of(step * STEP, STEP), STEP)
        for c in range(PEERS):
            for part in range(2):
                for half in range(2):
                    pair = [staged[sub, part, half, c * 8 : (c + 1) * 8, :] for sub in range(2)]
                    ready[c, part, rows, half * LANES : (half + 1) * LANES] = jnp.concatenate(pair, axis=0).astype(
                        jnp.bfloat16
                    )

    def send(step):
        rows = pl.ds(pl.multiple_of(step * STEP, STEP), STEP)
        there = pl.ds(pl.multiple_of(me * frames + step * STEP, STEP), STEP)
        for index, (dz, dx) in enumerate(OFFSETS):
            target = peer(me, dz, dx)
            pltpu.make_async_remote_copy(
                ready.at[target, :, rows],
                o_ref.at[:, there],
                send_sem.at[index],
                recv_sem.at[index],
                device_id={"tm": target},
                device_id_type=MESH,
            ).start()
        pltpu.make_async_copy(ready.at[me, :, rows], o_ref.at[:, there], send_sem.at[len(OFFSETS)]).start()

    compute(first_step)
    send(first_step)

    @pl.when(me == 0)
    def _():
        x[pl.ds(0, RIM_ROWS), :] = jnp.zeros((RIM_ROWS, LANES), jnp.float32)

    for copy in late:
        copy.wait()

    def step_body(i, carry):
        step = lax.rem(i + first_step, steps)

        @pl.when(jnp.logical_and(i == steps - first_step, odd))
        def _():
            rim_whole.wait_recv()

        @pl.when(jnp.logical_and(i == steps - first_step, even_gets))
        def _():
            rim_direct.wait_recv()
            rim_onward.wait_recv()

        compute(step)

        @pl.when(jnp.logical_and(i == 4, even_relays))
        def _():
            rim_aside.wait_recv()
            rim_onward.start()

        send(step)
        return carry

    lax.fori_loop(1, steps, step_body, 0)

    @pl.when(even)
    def _():
        rim_whole.wait_send()

    @pl.when(odd_sends)
    def _():
        rim_direct.wait_send()
        rim_aside.wait_send()

    @pl.when(even_relays)
    def _():
        rim_onward.wait_send()

    mine = pl.ds(pl.multiple_of(me * frames, STEP), frames)
    pltpu.make_async_copy(ready.at[me], o_ref.at[:, mine], send_sem.at[len(OFFSETS)]).wait()
    for index, (dz, dx) in enumerate(OFFSETS):
        target = peer(me, dz, dx)
        source = peer(me, -dz, dx)
        here = pl.ds(pl.multiple_of(source * frames, STEP), frames)
        whole = pltpu.make_async_remote_copy(
            ready.at[target],
            o_ref.at[:, here],
            send_sem.at[index],
            recv_sem.at[index],
            device_id={"tm": target},
            device_id_type=MESH,
        )
        whole.wait_send()
        whole.wait_recv()


def local(samples, prototype):
    block_len = samples.shape[1]
    frames = block_len // HOP
    rows = 2 * block_len // LANES
    x = samples.reshape(2, block_len // LANES, LANES).transpose(1, 0, 2).reshape(rows, LANES)
    one = jnp.concatenate([jnp.asarray(part) for part in first_matrix()], axis=0)
    two = jnp.concatenate([jnp.asarray(part) for part in second_matrix()], axis=0)
    mid = jnp.asarray(middle_tables())
    width = CHANNELS // PEERS

    def body(*refs):
        kernel(frames, *refs)

    return pl.pallas_call(
        body,
        out_shape=jax.ShapeDtypeStruct((2, PEERS * frames, width), jnp.bfloat16),
        in_specs=[pl.BlockSpec(memory_space=pltpu.HBM)] * 5,
        out_specs=pl.BlockSpec(memory_space=pltpu.HBM),
        scratch_shapes=[
            pltpu.VMEM((RIM_ROWS + rows, LANES), jnp.float32),
            pltpu.VMEM((RIM_ROWS // 2, LANES), jnp.float32),
            pltpu.VMEM((TAPS, CHANNELS), jnp.float32),
            pltpu.VMEM((TAPS * FRAME_ROWS, LANES), jnp.float32),
            pltpu.VMEM((512, 256), jnp.bfloat16),
            pltpu.VMEM((256, LANES), jnp.float32),
            pltpu.VMEM((512, 256), jnp.bfloat16),
            pltpu.VMEM((256, 256), jnp.bfloat16),
            pltpu.VMEM((256, 256), jnp.bfloat16),
            pltpu.VMEM((256, 256), jnp.bfloat16),
            pltpu.VMEM((256, 256), jnp.bfloat16),
            pltpu.VMEM((2, 2, 2, 128, LANES), jnp.float32),
            pltpu.VMEM((PEERS, 2, frames, width), jnp.bfloat16),
            pltpu.SemaphoreType.DMA((7,)),
            pltpu.SemaphoreType.DMA((2, 4)),
            pltpu.SemaphoreType.DMA((len(OFFSETS) + 1,)),
            pltpu.SemaphoreType.DMA((len(OFFSETS),)),
        ],
        compiler_params=pltpu.CompilerParams(
            collective_id=0, has_side_effects=True, vmem_limit_bytes=40 * 1024 * 1024
        ),
    )(*[pltpu.with_memory_space_constraint(value, pltpu.HBM) for value in (x, prototype, one, mid, two)])


def solution(mesh):
    placed = (P(None, ("beam", "tm")), P())
    return jax.shard_map(
        local, mesh=mesh, in_specs=placed, out_specs=P(None, "beam", "tm"), check_vma=False
    )
```

```python
import math

import jax
import jax.numpy as jnp
import numpy as np
from jax import lax
from jax.experimental import pallas as pl
from jax.experimental.pallas import tpu as pltpu
from jax.sharding import PartitionSpec as P

CHANNELS = 4096
TAPS = 16
HOP = 3072
LANES = 128
ROWS = 32
PEERS = 16
FRAME_ROWS = 2 * ROWS
HOP_ROWS = 2 * HOP // LANES
RIM_ROWS = 2 * (TAPS * CHANNELS - HOP) // LANES
STEP = 16
ASIDE_FIRST, ASIDE_COUNT, ASIDE_ONWARD = 2, 2, 7
MESH = pl.DeviceIdType.MESH
OFFSETS = [(dz, dx) for dz in (4, 3, -3, 2, -2, 1, -1) for dx in (1, 0)] + [(0, 1)]


def split_bf16(table):
    high = table.astype(np.float32).astype(jnp.bfloat16)
    low = (table - high.astype(np.float64)).astype(np.float32).astype(jnp.bfloat16)
    return high, low


def first_matrix():
    a = np.arange(ROWS)
    table = np.zeros((2, 4, ROWS, 4, ROWS, 2))
    for frame in range(4):
        turns = (-np.outer(a, a) + 8 * a[:, None] * (frame + 1)) % 32
        unit = np.exp(2j * np.pi * turns / 32) / 64
        table[0, frame, :, frame, :, 0] = unit.real
        table[0, frame, :, frame, :, 1] = -unit.imag
        table[1, frame, :, frame, :, 0] = unit.imag
        table[1, frame, :, frame, :, 1] = unit.real
    return split_bf16(table.reshape(256, 256))


def middle_tables():
    turns = np.outer(np.arange(ROWS), np.arange(LANES))
    angle = 2 * np.pi * turns / CHANNELS
    tables = np.stack([np.cos(angle), np.sin(angle)])
    return np.tile(tables, (1, 4, 1)).reshape(256, LANES).astype(np.float32)


def second_matrix():
    k_l = (8 * np.arange(16)[None, :] + np.arange(8)[:, None]).reshape(-1)
    angle = 2 * np.pi * (np.outer(k_l, np.arange(LANES)) % LANES) / LANES
    c, s = np.cos(angle), np.sin(angle)
    return split_bf16(np.block([[c, s], [-s, c]]))


def peer(me, dz, dx):
    return (me // 2 + dz + 8) % 8 * 2 + (me % 2 + dx) % 2


def dot3(left_high, left_low, right_high, right_low, dims):
    def one(a, b):
        return lax.dot_general(a, b, (dims, ((), ())), preferred_element_type=jnp.float32)

    return one(left_high, right_high) + one(left_high, right_low) + one(left_low, right_high)


def halves(value):
    high = value.astype(jnp.bfloat16)
    return high, (value - high.astype(jnp.float32)).astype(jnp.bfloat16)


def kernel(
    frames, x_hbm, h_hbm, one_hbm, mid_hbm, two_hbm, o_ref,
    x, rim_relay, far_relay, taps_in, h, one, mid, two, fold_high, fold_low, turn_high, turn_low, staged, ready,
    load_sem, rim_sem, far_sem, send_sem, recv_sem,
):
    me = lax.axis_index("tm")
    local_rows = frames * HOP_ROWS
    steps = frames // STEP
    first_step = 2
    low_row = first_step * STEP * HOP_ROWS - RIM_ROWS
    high_row = ((first_step + 1) * STEP - 1) * HOP_ROWS + TAPS * FRAME_ROWS - RIM_ROWS

    barrier = pltpu.get_barrier_semaphore()
    for dz, dx in OFFSETS:
        pl.semaphore_signal(barrier, inc=1, device_id={"tm": peer(me, dz, dx)}, device_id_type=MESH)

    def load(index, start, stop):
        return pltpu.make_async_copy(
            x_hbm.at[pl.ds(start, stop - start)], x.at[pl.ds(RIM_ROWS + start, stop - start)], load_sem.at[index]
        )

    early = [
        load(0, low_row, high_row),
        pltpu.make_async_copy(h_hbm, taps_in, load_sem.at[3]),
        pltpu.make_async_copy(one_hbm, one, load_sem.at[4]),
        pltpu.make_async_copy(mid_hbm, mid, load_sem.at[5]),
        pltpu.make_async_copy(two_hbm, two, load_sem.at[6]),
    ]
    late = [load(1, high_row, local_rows), load(2, 0, low_row)]
    for copy in early + late:
        copy.start()

    half_rim = RIM_ROWS // 2
    rim_start = local_rows - RIM_ROWS

    def rim(index, source, place, steps_on):
        return pltpu.make_async_remote_copy(
            source,
            place,
            rim_sem.at[0, index],
            rim_sem.at[1, index],
            device_id={"tm": lax.rem(me + steps_on + PEERS, PEERS)},
            device_id_type=MESH,
        )

    rim_whole = rim(0, x_hbm.at[pl.ds(rim_start, RIM_ROWS)], x.at[pl.ds(0, RIM_ROWS)], 1)
    rim_direct = rim(1, x_hbm.at[pl.ds(rim_start, half_rim)], x.at[pl.ds(0, half_rim)], 1)
    rim_aside = rim(2, x_hbm.at[pl.ds(rim_start + half_rim, half_rim)], rim_relay, -1)
    rim_onward = rim(3, rim_relay, x.at[pl.ds(half_rim, half_rim)], 2)
    odd = lax.rem(me, 2) == 1
    even = lax.rem(me, 2) == 0
    odd_sends = jnp.logical_and(odd, me < PEERS - 1)
    even_relays = jnp.logical_and(even, me < PEERS - 2)
    even_gets = jnp.logical_and(even, me > 0)

    for copy in early:
        copy.wait()

    for a in range(ROWS):
        for part in range(2):
            h[pl.ds(2 * a + part, TAPS, stride=FRAME_ROWS), :] = taps_in[:, a * LANES : (a + 1) * LANES]

    lane = lax.broadcasted_iota(jnp.int32, (16, LANES), 1)
    low_64 = lane < 64
    even_32 = lane // 32 % 2 == 0

    def exchange(tiles):
        a, b, c, d = tiles
        ac = jnp.where(low_64, a, pltpu.roll(c, 64, 1)), jnp.where(low_64, pltpu.roll(a, 64, 1), c)
        bd = jnp.where(low_64, b, pltpu.roll(d, 64, 1)), jnp.where(low_64, pltpu.roll(b, 64, 1), d)
        done = []
        for p, q in zip(ac, bd):
            done.append(jnp.where(even_32, p, pltpu.roll(q, 32, 1)))
            done.append(jnp.where(even_32, pltpu.roll(p, 96, 1), q))
        return done

    def eight_frames(first_frame, sub):
        base = first_frame * HOP_ROWS

        def fold(block, carry):
            at = pl.multiple_of(block * 16, 16)
            taps = [h[pl.ds(at + p * FRAME_ROWS, 16), :] for p in range(TAPS)]
            for f in range(8):
                total = None
                for p in range(TAPS):
                    rows = pl.ds(pl.multiple_of(base + f * HOP_ROWS + p * FRAME_ROWS + at, 16), 16)
                    term = taps[p] * x[rows, :]
                    total = term if total is None else total + term
                high, low = halves(total)
                place = pl.ds(pl.multiple_of(f % 4 * FRAME_ROWS + at, 16), 16)
                fold_high[place, f // 4 * LANES : (f // 4 + 1) * LANES] = high
                fold_low[place, f // 4 * LANES : (f // 4 + 1) * LANES] = low
            return carry

        lax.fori_loop(0, FRAME_ROWS // 16, fold, 0)

        section = dot3(one[0:256, :], one[256:512, :], fold_high[...], fold_low[...], ((1,), (0,)))
        cos_mid, sin_mid = mid[0:128, :], mid[128:256, :]
        for g in range(2):
            re = section[0:128, g * LANES : (g + 1) * LANES]
            im = section[128:256, g * LANES : (g + 1) * LANES]
            for part, value in enumerate((re * cos_mid + im * sin_mid, im * cos_mid - re * sin_mid)):
                high, low = halves(value)
                turn_high[g * 128 : (g + 1) * 128, part * LANES : (part + 1) * LANES] = high
                turn_low[g * 128 : (g + 1) * 128, part * LANES : (part + 1) * LANES] = low

        out = dot3(two[0:256, :], two[256:512, :], turn_high[...], turn_low[...], ((1,), (1,)))
        for part in range(2):
            for half in range(2):
                for side in range(2):
                    tiles = [
                        out[part * 128 + (half * 4 + q) * 16 : part * 128 + (half * 4 + q + 1) * 16,
                            side * LANES : (side + 1) * LANES]
                        for q in range(4)
                    ]
                    for r, tile in enumerate(exchange(tiles)):
                        staged[sub, part, half, pl.ds(side * 4 + r, 16, stride=8), :] = tile

    def compute(step, between=None):
        for sub in range(2):
            eight_frames(step * STEP + sub * 8, sub)
            if sub == 0 and between is not None:
                between()

        rows = pl.ds(pl.multiple_of(step * STEP, STEP), STEP)
        for c in range(PEERS):
            for part in range(2):
                for half in range(2):
                    pair = [staged[sub, part, half, c * 8 : (c + 1) * 8, :] for sub in range(2)]
                    ready[c, part, rows, half * LANES : (half + 1) * LANES] = jnp.concatenate(pair, axis=0).astype(
                        jnp.bfloat16
                    )

    def direct(step, index):
        dz, dx = OFFSETS[index]
        rows = pl.ds(pl.multiple_of(step * STEP, STEP), STEP)
        target = peer(me, dz, dx)
        return pltpu.make_async_remote_copy(
            ready.at[target, :, rows],
            o_ref.at[:, pl.ds(pl.multiple_of(me * frames + step * STEP, STEP), STEP)],
            send_sem.at[index],
            recv_sem.at[index],
            device_id={"tm": target},
            device_id_type=MESH,
        )

    z_even = lax.rem(me // 2, 2) == 0
    z_odd = lax.rem(me // 2, 2) == 1

    def far_aside(step, slot, dx):
        rows = pl.ds(pl.multiple_of(step * STEP, STEP), STEP)
        return pltpu.make_async_remote_copy(
            ready.at[peer(me, 4, dx), :, rows],
            far_relay.at[slot, dx],
            send_sem.at[OFFSETS.index((4, dx))],
            far_sem.at[1, slot, dx],
            device_id={"tm": peer(me, -1, 0)},
            device_id_type=MESH,
        )

    def far_onward(slot, dx):
        source = peer(me, 1, 0)
        step = slot + ASIDE_FIRST + first_step
        return pltpu.make_async_remote_copy(
            far_relay.at[slot, dx],
            o_ref.at[:, pl.ds(pl.multiple_of(source * frames + step * STEP, STEP), STEP)],
            far_sem.at[0, slot, dx],
            recv_sem.at[OFFSETS.index((4, dx))],
            device_id={"tm": peer(me, -3, dx)},
            device_id_type=MESH,
        )

    def send(step, aside=None):
        for index, (dz, dx) in enumerate(OFFSETS):
            if dz == 4 and aside is not None:
                for slot in range(ASIDE_COUNT):
                    @pl.when(jnp.logical_and(aside == slot, z_even))
                    def _():
                        far_aside(step, slot, dx).start()

                @pl.when(jnp.logical_or(jnp.logical_or(aside < 0, aside >= ASIDE_COUNT), z_odd))
                def _():
                    direct(step, index).start()
            else:
                direct(step, index).start()
        rows = pl.ds(pl.multiple_of(step * STEP, STEP), STEP)
        there = pl.ds(pl.multiple_of(me * frames + step * STEP, STEP), STEP)
        pltpu.make_async_copy(ready.at[me, :, rows], o_ref.at[:, there], send_sem.at[len(OFFSETS)]).start()

    def meet():
        pl.semaphore_wait(barrier, len(OFFSETS))

        @pl.when(even)
        def _():
            rim_whole.start()

        @pl.when(odd_sends)
        def _():
            rim_direct.start()
            rim_aside.start()

    compute(first_step, meet)
    send(first_step)

    @pl.when(me == 0)
    def _():
        x[pl.ds(0, RIM_ROWS), :] = jnp.zeros((RIM_ROWS, LANES), jnp.float32)

    for copy in late:
        copy.wait()

    def step_body(i, carry):
        step = lax.rem(i + first_step, steps)

        @pl.when(jnp.logical_and(i == steps - first_step, odd))
        def _():
            rim_whole.wait_recv()

        @pl.when(jnp.logical_and(i == steps - first_step, even_gets))
        def _():
            rim_direct.wait_recv()
            rim_onward.wait_recv()

        compute(step)

        @pl.when(jnp.logical_and(i == 4, even_relays))
        def _():
            rim_aside.wait_recv()
            rim_onward.start()

        @pl.when(jnp.logical_and(i == ASIDE_ONWARD, z_odd))
        def _():
            for slot in range(ASIDE_COUNT):
                for dx in range(2):
                    far_aside(step, slot, dx).wait_recv()
                    far_onward(slot, dx).start()

        send(step, i - ASIDE_FIRST)
        return carry

    lax.fori_loop(1, steps, step_body, 0)

    @pl.when(even)
    def _():
        rim_whole.wait_send()

    @pl.when(odd_sends)
    def _():
        rim_direct.wait_send()
        rim_aside.wait_send()

    @pl.when(even_relays)
    def _():
        rim_onward.wait_send()

    @pl.when(z_odd)
    def _():
        for slot in range(ASIDE_COUNT):
            for dx in range(2):
                far_onward(slot, dx).wait_send()

    mine = pl.ds(pl.multiple_of(me * frames, STEP), frames)
    pltpu.make_async_copy(ready.at[me], o_ref.at[:, mine], send_sem.at[len(OFFSETS)]).wait()
    for index, (dz, dx) in enumerate(OFFSETS):
        target = peer(me, dz, dx)
        source = peer(me, -dz, dx)
        here = pl.ds(pl.multiple_of(source * frames, STEP), frames)
        whole = pltpu.make_async_remote_copy(
            ready.at[target],
            o_ref.at[:, here],
            send_sem.at[index],
            recv_sem.at[index],
            device_id={"tm": target},
            device_id_type=MESH,
        )
        whole.wait_send()
        whole.wait_recv()


def local(samples, prototype):
    block_len = samples.shape[1]
    frames = block_len // HOP
    rows = 2 * block_len // LANES
    x = samples.reshape(2, block_len // LANES, LANES).transpose(1, 0, 2).reshape(rows, LANES)
    one = jnp.concatenate([jnp.asarray(part) for part in first_matrix()], axis=0)
    two = jnp.concatenate([jnp.asarray(part) for part in second_matrix()], axis=0)
    mid = jnp.asarray(middle_tables())
    width = CHANNELS // PEERS

    def body(*refs):
        kernel(frames, *refs)

    return pl.pallas_call(
        body,
        out_shape=jax.ShapeDtypeStruct((2, PEERS * frames, width), jnp.bfloat16),
        in_specs=[pl.BlockSpec(memory_space=pltpu.HBM)] * 5,
        out_specs=pl.BlockSpec(memory_space=pltpu.HBM),
        scratch_shapes=[
            pltpu.VMEM((RIM_ROWS + rows, LANES), jnp.float32),
            pltpu.VMEM((RIM_ROWS // 2, LANES), jnp.float32),
            pltpu.VMEM((ASIDE_COUNT, 2, 2, STEP, width), jnp.bfloat16),
            pltpu.VMEM((TAPS, CHANNELS), jnp.float32),
            pltpu.VMEM((TAPS * FRAME_ROWS, LANES), jnp.float32),
            pltpu.VMEM((512, 256), jnp.bfloat16),
            pltpu.VMEM((256, LANES), jnp.float32),
            pltpu.VMEM((512, 256), jnp.bfloat16),
            pltpu.VMEM((256, 256), jnp.bfloat16),
            pltpu.VMEM((256, 256), jnp.bfloat16),
            pltpu.VMEM((256, 256), jnp.bfloat16),
            pltpu.VMEM((256, 256), jnp.bfloat16),
            pltpu.VMEM((2, 2, 2, 128, LANES), jnp.float32),
            pltpu.VMEM((PEERS, 2, frames, width), jnp.bfloat16),
            pltpu.SemaphoreType.DMA((7,)),
            pltpu.SemaphoreType.DMA((2, 4)),
            pltpu.SemaphoreType.DMA((2, ASIDE_COUNT, 2)),
            pltpu.SemaphoreType.DMA((len(OFFSETS) + 1,)),
            pltpu.SemaphoreType.DMA((len(OFFSETS),)),
        ],
        compiler_params=pltpu.CompilerParams(
            collective_id=0, has_side_effects=True, vmem_limit_bytes=40 * 1024 * 1024
        ),
    )(*[pltpu.with_memory_space_constraint(value, pltpu.HBM) for value in (x, prototype, one, mid, two)])


def solution(mesh):
    placed = (P(None, ("beam", "tm")), P())
    return jax.shard_map(
        local, mesh=mesh, in_specs=placed, out_specs=P(None, "beam", "tm"), check_vma=False
    )
```

```python
import math

import jax
import jax.numpy as jnp
import numpy as np
from jax import lax
from jax.experimental import pallas as pl
from jax.experimental.pallas import tpu as pltpu
from jax.sharding import PartitionSpec as P

CHANNELS = 4096
TAPS = 16
HOP = 3072
LANES = 128
ROWS = 32
PEERS = 16
FRAME_ROWS = 2 * ROWS
HOP_ROWS = 2 * HOP // LANES
RIM_ROWS = 2 * (TAPS * CHANNELS - HOP) // LANES
STEP = 16
ASIDE_FIRST, ASIDE_COUNT, ASIDE_ONWARD = 5, 2, 9
MESH = pl.DeviceIdType.MESH
OFFSETS = [(dz, dx) for dz in (4, 3, -3, 2, -2, 1, -1) for dx in (1, 0)] + [(0, 1)]


def split_bf16(table):
    high = table.astype(np.float32).astype(jnp.bfloat16)
    low = (table - high.astype(np.float64)).astype(np.float32).astype(jnp.bfloat16)
    return high, low


def first_matrix():
    a = np.arange(ROWS)
    table = np.zeros((2, 4, ROWS, 4, ROWS, 2))
    for frame in range(4):
        turns = (-np.outer(a, a) + 8 * a[:, None] * (frame + 1)) % 32
        unit = np.exp(2j * np.pi * turns / 32) / 64
        table[0, frame, :, frame, :, 0] = unit.real
        table[0, frame, :, frame, :, 1] = -unit.imag
        table[1, frame, :, frame, :, 0] = unit.imag
        table[1, frame, :, frame, :, 1] = unit.real
    return split_bf16(table.reshape(256, 256))


def middle_tables():
    turns = np.outer(np.arange(ROWS), np.arange(LANES))
    angle = 2 * np.pi * turns / CHANNELS
    tables = np.stack([np.cos(angle), np.sin(angle)])
    return np.tile(tables, (1, 4, 1)).reshape(256, LANES).astype(np.float32)


def second_matrix():
    k_l = (8 * np.arange(16)[None, :] + np.arange(8)[:, None]).reshape(-1)
    angle = 2 * np.pi * (np.outer(k_l, np.arange(LANES)) % LANES) / LANES
    c, s = np.cos(angle), np.sin(angle)
    return split_bf16(np.block([[c, s], [-s, c]]))


def peer(me, dz, dx):
    return (me // 2 + dz + 8) % 8 * 2 + (me % 2 + dx) % 2


def dot3(left_high, left_low, right_high, right_low, dims):
    def one(a, b):
        return lax.dot_general(a, b, (dims, ((), ())), preferred_element_type=jnp.float32)

    return one(left_high, right_high) + one(left_high, right_low) + one(left_low, right_high)


def halves(value):
    high = value.astype(jnp.bfloat16)
    return high, (value - high.astype(jnp.float32)).astype(jnp.bfloat16)


def kernel(
    frames, x_hbm, h_hbm, one_hbm, mid_hbm, two_hbm, o_ref,
    x, rim_relay, far_relay, taps_in, h, one, mid, two, fold_high, fold_low, turn_high, turn_low, staged, ready,
    load_sem, rim_sem, far_sem, send_sem, recv_sem,
):
    me = lax.axis_index("tm")
    local_rows = frames * HOP_ROWS
    steps = frames // STEP
    first_step = 2
    low_row = first_step * STEP * HOP_ROWS - RIM_ROWS
    high_row = ((first_step + 1) * STEP - 1) * HOP_ROWS + TAPS * FRAME_ROWS - RIM_ROWS

    barrier = pltpu.get_barrier_semaphore()
    for dz, dx in OFFSETS:
        pl.semaphore_signal(barrier, inc=1, device_id={"tm": peer(me, dz, dx)}, device_id_type=MESH)

    def load(index, start, stop):
        return pltpu.make_async_copy(
            x_hbm.at[pl.ds(start, stop - start)], x.at[pl.ds(RIM_ROWS + start, stop - start)], load_sem.at[index]
        )

    early = [
        load(0, low_row, high_row),
        pltpu.make_async_copy(h_hbm, taps_in, load_sem.at[3]),
        pltpu.make_async_copy(one_hbm, one, load_sem.at[4]),
        pltpu.make_async_copy(mid_hbm, mid, load_sem.at[5]),
        pltpu.make_async_copy(two_hbm, two, load_sem.at[6]),
    ]
    late = [load(1, high_row, local_rows), load(2, 0, low_row)]
    for copy in early + late:
        copy.start()

    half_rim = RIM_ROWS // 2
    rim_start = local_rows - RIM_ROWS

    def rim(index, source, place, steps_on):
        return pltpu.make_async_remote_copy(
            source,
            place,
            rim_sem.at[0, index],
            rim_sem.at[1, index],
            device_id={"tm": lax.rem(me + steps_on + PEERS, PEERS)},
            device_id_type=MESH,
        )

    rim_whole = rim(0, x_hbm.at[pl.ds(rim_start, RIM_ROWS)], x.at[pl.ds(0, RIM_ROWS)], 1)
    rim_direct = rim(1, x_hbm.at[pl.ds(rim_start, half_rim)], x.at[pl.ds(0, half_rim)], 1)
    rim_aside = rim(2, x_hbm.at[pl.ds(rim_start + half_rim, half_rim)], rim_relay, -1)
    rim_onward = rim(3, rim_relay, x.at[pl.ds(half_rim, half_rim)], 2)
    odd = lax.rem(me, 2) == 1
    even = lax.rem(me, 2) == 0
    odd_sends = jnp.logical_and(odd, me < PEERS - 1)
    even_relays = jnp.logical_and(even, me < PEERS - 2)
    even_gets = jnp.logical_and(even, me > 0)

    for copy in early:
        copy.wait()

    for a in range(ROWS):
        for part in range(2):
            h[pl.ds(2 * a + part, TAPS, stride=FRAME_ROWS), :] = taps_in[:, a * LANES : (a + 1) * LANES]

    lane = lax.broadcasted_iota(jnp.int32, (16, LANES), 1)
    low_64 = lane < 64
    even_32 = lane // 32 % 2 == 0

    def exchange(tiles):
        a, b, c, d = tiles
        ac = jnp.where(low_64, a, pltpu.roll(c, 64, 1)), jnp.where(low_64, pltpu.roll(a, 64, 1), c)
        bd = jnp.where(low_64, b, pltpu.roll(d, 64, 1)), jnp.where(low_64, pltpu.roll(b, 64, 1), d)
        done = []
        for p, q in zip(ac, bd):
            done.append(jnp.where(even_32, p, pltpu.roll(q, 32, 1)))
            done.append(jnp.where(even_32, pltpu.roll(p, 96, 1), q))
        return done

    def eight_frames(first_frame, sub):
        base = first_frame * HOP_ROWS

        def fold(block, carry):
            at = pl.multiple_of(block * 16, 16)
            taps = [h[pl.ds(at + p * FRAME_ROWS, 16), :] for p in range(TAPS)]
            for f in range(8):
                total = None
                for p in range(TAPS):
                    rows = pl.ds(pl.multiple_of(base + f * HOP_ROWS + p * FRAME_ROWS + at, 16), 16)
                    term = taps[p] * x[rows, :]
                    total = term if total is None else total + term
                high, low = halves(total)
                place = pl.ds(pl.multiple_of(f % 4 * FRAME_ROWS + at, 16), 16)
                fold_high[place, f // 4 * LANES : (f // 4 + 1) * LANES] = high
                fold_low[place, f // 4 * LANES : (f // 4 + 1) * LANES] = low
            return carry

        lax.fori_loop(0, FRAME_ROWS // 16, fold, 0)

        section = dot3(one[0:256, :], one[256:512, :], fold_high[...], fold_low[...], ((1,), (0,)))
        cos_mid, sin_mid = mid[0:128, :], mid[128:256, :]
        for g in range(2):
            re = section[0:128, g * LANES : (g + 1) * LANES]
            im = section[128:256, g * LANES : (g + 1) * LANES]
            for part, value in enumerate((re * cos_mid + im * sin_mid, im * cos_mid - re * sin_mid)):
                high, low = halves(value)
                turn_high[g * 128 : (g + 1) * 128, part * LANES : (part + 1) * LANES] = high
                turn_low[g * 128 : (g + 1) * 128, part * LANES : (part + 1) * LANES] = low

        out = dot3(two[0:256, :], two[256:512, :], turn_high[...], turn_low[...], ((1,), (1,)))
        for part in range(2):
            for half in range(2):
                for side in range(2):
                    tiles = [
                        out[part * 128 + (half * 4 + q) * 16 : part * 128 + (half * 4 + q + 1) * 16,
                            side * LANES : (side + 1) * LANES]
                        for q in range(4)
                    ]
                    for r, tile in enumerate(exchange(tiles)):
                        staged[sub, part, half, pl.ds(side * 4 + r, 16, stride=8), :] = tile

    def compute(step, between=None):
        for sub in range(2):
            eight_frames(step * STEP + sub * 8, sub)
            if sub == 0 and between is not None:
                between()

        rows = pl.ds(pl.multiple_of(step * STEP, STEP), STEP)
        for c in range(PEERS):
            for part in range(2):
                for half in range(2):
                    pair = [staged[sub, part, half, c * 8 : (c + 1) * 8, :] for sub in range(2)]
                    ready[c, part, rows, half * LANES : (half + 1) * LANES] = jnp.concatenate(pair, axis=0).astype(
                        jnp.bfloat16
                    )

    def direct(step, index):
        dz, dx = OFFSETS[index]
        rows = pl.ds(pl.multiple_of(step * STEP, STEP), STEP)
        target = peer(me, dz, dx)
        return pltpu.make_async_remote_copy(
            ready.at[target, :, rows],
            o_ref.at[:, pl.ds(pl.multiple_of(me * frames + step * STEP, STEP), STEP)],
            send_sem.at[index],
            recv_sem.at[index],
            device_id={"tm": target},
            device_id_type=MESH,
        )

    z_even = lax.rem(me // 2, 2) == 0
    z_odd = lax.rem(me // 2, 2) == 1

    def far_aside(step, slot, dx):
        rows = pl.ds(pl.multiple_of(step * STEP, STEP), STEP)
        return pltpu.make_async_remote_copy(
            ready.at[peer(me, 4, dx), :, rows],
            far_relay.at[slot, dx],
            send_sem.at[OFFSETS.index((4, dx))],
            far_sem.at[1, slot, dx],
            device_id={"tm": peer(me, -1, 0)},
            device_id_type=MESH,
        )

    def far_onward(slot, dx):
        source = peer(me, 1, 0)
        step = slot + ASIDE_FIRST + first_step
        return pltpu.make_async_remote_copy(
            far_relay.at[slot, dx],
            o_ref.at[:, pl.ds(pl.multiple_of(source * frames + step * STEP, STEP), STEP)],
            far_sem.at[0, slot, dx],
            recv_sem.at[OFFSETS.index((4, dx))],
            device_id={"tm": peer(me, -3, dx)},
            device_id_type=MESH,
        )

    def send(step, aside=None):
        order = list(enumerate(OFFSETS))
        if aside is None:
            order.reverse()
        for index, (dz, dx) in order:
            if dz == 4 and aside is not None:
                for slot in range(ASIDE_COUNT):
                    @pl.when(jnp.logical_and(aside == slot, z_even))
                    def _():
                        far_aside(step, slot, dx).start()

                @pl.when(jnp.logical_or(jnp.logical_or(aside < 0, aside >= ASIDE_COUNT), z_odd))
                def _():
                    direct(step, index).start()
            else:
                direct(step, index).start()
        rows = pl.ds(pl.multiple_of(step * STEP, STEP), STEP)
        there = pl.ds(pl.multiple_of(me * frames + step * STEP, STEP), STEP)
        pltpu.make_async_copy(ready.at[me, :, rows], o_ref.at[:, there], send_sem.at[len(OFFSETS)]).start()

    def meet():
        pl.semaphore_wait(barrier, len(OFFSETS))

        @pl.when(even)
        def _():
            rim_whole.start()

        @pl.when(odd_sends)
        def _():
            rim_direct.start()
            rim_aside.start()

    compute(first_step, meet)
    send(first_step)

    @pl.when(me == 0)
    def _():
        x[pl.ds(0, RIM_ROWS), :] = jnp.zeros((RIM_ROWS, LANES), jnp.float32)

    for copy in late:
        copy.wait()

    def step_body(i, carry):
        step = lax.rem(i + first_step, steps)

        @pl.when(jnp.logical_and(i == steps - first_step, odd))
        def _():
            rim_whole.wait_recv()

        @pl.when(jnp.logical_and(i == steps - first_step, even_gets))
        def _():
            rim_direct.wait_recv()
            rim_onward.wait_recv()

        compute(step)

        @pl.when(jnp.logical_and(i == 4, even_relays))
        def _():
            rim_aside.wait_recv()
            rim_onward.start()

        @pl.when(jnp.logical_and(i == ASIDE_ONWARD, z_odd))
        def _():
            for slot in range(ASIDE_COUNT):
                for dx in range(2):
                    far_aside(step, slot, dx).wait_recv()
                    far_onward(slot, dx).start()

        send(step, i - ASIDE_FIRST)
        return carry

    lax.fori_loop(1, steps, step_body, 0)

    @pl.when(even)
    def _():
        rim_whole.wait_send()

    @pl.when(odd_sends)
    def _():
        rim_direct.wait_send()
        rim_aside.wait_send()

    @pl.when(even_relays)
    def _():
        rim_onward.wait_send()

    @pl.when(z_odd)
    def _():
        for slot in range(ASIDE_COUNT):
            for dx in range(2):
                far_onward(slot, dx).wait_send()

    mine = pl.ds(pl.multiple_of(me * frames, STEP), frames)
    pltpu.make_async_copy(ready.at[me], o_ref.at[:, mine], send_sem.at[len(OFFSETS)]).wait()
    for index, (dz, dx) in enumerate(OFFSETS):
        target = peer(me, dz, dx)
        source = peer(me, -dz, dx)
        here = pl.ds(pl.multiple_of(source * frames, STEP), frames)
        whole = pltpu.make_async_remote_copy(
            ready.at[target],
            o_ref.at[:, here],
            send_sem.at[index],
            recv_sem.at[index],
            device_id={"tm": target},
            device_id_type=MESH,
        )
        whole.wait_send()
        whole.wait_recv()


def local(samples, prototype):
    block_len = samples.shape[1]
    frames = block_len // HOP
    rows = 2 * block_len // LANES
    x = samples.reshape(2, block_len // LANES, LANES).transpose(1, 0, 2).reshape(rows, LANES)
    one = jnp.concatenate([jnp.asarray(part) for part in first_matrix()], axis=0)
    two = jnp.concatenate([jnp.asarray(part) for part in second_matrix()], axis=0)
    mid = jnp.asarray(middle_tables())
    width = CHANNELS // PEERS

    def body(*refs):
        kernel(frames, *refs)

    return pl.pallas_call(
        body,
        out_shape=jax.ShapeDtypeStruct((2, PEERS * frames, width), jnp.bfloat16),
        in_specs=[pl.BlockSpec(memory_space=pltpu.HBM)] * 5,
        out_specs=pl.BlockSpec(memory_space=pltpu.HBM),
        scratch_shapes=[
            pltpu.VMEM((RIM_ROWS + rows, LANES), jnp.float32),
            pltpu.VMEM((RIM_ROWS // 2, LANES), jnp.float32),
            pltpu.VMEM((ASIDE_COUNT, 2, 2, STEP, width), jnp.bfloat16),
            pltpu.VMEM((TAPS, CHANNELS), jnp.float32),
            pltpu.VMEM((TAPS * FRAME_ROWS, LANES), jnp.float32),
            pltpu.VMEM((512, 256), jnp.bfloat16),
            pltpu.VMEM((256, LANES), jnp.float32),
            pltpu.VMEM((512, 256), jnp.bfloat16),
            pltpu.VMEM((256, 256), jnp.bfloat16),
            pltpu.VMEM((256, 256), jnp.bfloat16),
            pltpu.VMEM((256, 256), jnp.bfloat16),
            pltpu.VMEM((256, 256), jnp.bfloat16),
            pltpu.VMEM((2, 2, 2, 128, LANES), jnp.float32),
            pltpu.VMEM((PEERS, 2, frames, width), jnp.bfloat16),
            pltpu.SemaphoreType.DMA((7,)),
            pltpu.SemaphoreType.DMA((2, 4)),
            pltpu.SemaphoreType.DMA((2, ASIDE_COUNT, 2)),
            pltpu.SemaphoreType.DMA((len(OFFSETS) + 1,)),
            pltpu.SemaphoreType.DMA((len(OFFSETS),)),
        ],
        compiler_params=pltpu.CompilerParams(
            collective_id=0, has_side_effects=True, vmem_limit_bytes=40 * 1024 * 1024
        ),
    )(*[pltpu.with_memory_space_constraint(value, pltpu.HBM) for value in (x, prototype, one, mid, two)])


def solution(mesh):
    placed = (P(None, ("beam", "tm")), P())
    return jax.shard_map(
        local, mesh=mesh, in_specs=placed, out_specs=P(None, "beam", "tm"), check_vma=False
    )
```
